32 devices in a mesh: gx: 8 (over y, x, core), gy: 4 (over z).
Axes of the slice: x: 2, y: 2, z: 4, core: 2. Of those that a mesh axis runs over, the one named last changes fastest.
Arguments:
- source_field: bfloat16 [4096, 128, 128], P(('gx', 'gy')), may hold values from -6 to 6
- weight_blocks: bfloat16 [16384, 128, 128], P(('gx', 'gy')), may hold values from -0.1875 to 0.1875
- source_ids: int32 [16384], replicated, may hold values from 0 to 4095, as said below
- target_ids: int32 [16384], replicated, may hold values from 0 to 2047, as said below
Outputs:
- remapped: bfloat16 [2048, 128, 128], P(('gx', 'gy'))
The draws below stay inside these ranges and needn't reach their ends.
Inputs may be any that keep to these rules, and one draw needn't show every extreme that they name: `source_ids`: source block b lies on device b // 128 of gx+gy, and weight block k lies on device k // 512. The weight blocks of device d name only source blocks of devices d - 2 to d + 2. Among the weight blocks of one device, at most 64 distinct source blocks of any one other device are named, and exactly 64 for some other device. `target_ids`: target block t lies on device t // 64 of gx+gy. The weight blocks of device d name only target blocks of devices d - 2 to d + 2. Among the weight blocks of one device, at most 16 distinct target blocks of any one device are named, and exactly 16 for some other device.
All inputs are finite; a program needn't handle non-finite values.
Results may differ from the reference program's by a relative error of at most 0.001.
Values may be sent and summed in bfloat16 or wider, within the bound.
No kernel may reach another device: no remote copies, remote signals or barrier semaphores. Data moves between devices by JAX's collectives and lax.ppermute only.
A program may use at most 192 MiB of HBM per device.

```python
import jax
import jax.numpy as jnp
from jax import lax

BLK = 128
CH = 128
HALF = 2
SB_DEV = 128
TB_DEV = 64
WB_DEV = 512
CAP_S = 64
CAP_T = 16
NSB = 4096
NW = 16384
N_GX = 8
N_GY = 4


def pair_ids(key, slot_count, per_device):
    devices = N_GX * N_GY
    span = 2 * HALF + 1

    def one_device(device):
        keyed = jax.random.fold_in(key, device)
        key_count, key_force, key_perm, key_pick, key_order = jax.random.split(keyed, 5)
        offsets = jnp.arange(span, dtype=jnp.int32) - HALF
        owner = device + offsets
        valid = (owner >= 0) & (owner < devices)
        counts = jax.random.randint(key_count, (span,), slot_count // 2, slot_count + 1)
        scores = jax.random.randint(key_force, (span,), 0, 1024) * span + jnp.arange(span, dtype=jnp.int32)
        scores = jnp.where(valid & (offsets != 0), scores, -1)
        forced = jnp.argmax(scores)
        counts = jnp.where((jnp.arange(span, dtype=jnp.int32) == forced) | (offsets == 0), slot_count, counts)
        counts = jnp.where(valid, counts, 0)
        perms = jax.vmap(lambda kk: jax.random.permutation(kk, per_device))(jax.random.split(key_perm, span))
        chosen = perms[:, :slot_count].reshape(-1)
        used = (jnp.arange(slot_count, dtype=jnp.int32)[None, :] < counts[:, None]).reshape(-1)
        entries = span * slot_count
        block_index = jnp.arange(WB_DEV, dtype=jnp.int32)
        picked = jax.random.randint(key_pick, (WB_DEV,), 0, entries)
        entry = jnp.where(block_index < entries, block_index, picked)
        entry = jnp.where(used[entry], entry, HALF * slot_count + entry % slot_count)
        order = jax.random.permutation(key_order, WB_DEV)
        entry = entry[order]
        return (owner[entry // slot_count] * per_device + chosen[entry]).astype(jnp.int32)
    return jax.vmap(one_device)(jnp.arange(devices, dtype=jnp.int32)).reshape(-1).astype(jnp.int32)


def draw_source_ids(key, part):
    return pair_ids(jax.random.fold_in(key, 11), CAP_S, SB_DEV)


def draw_target_ids(key, part):
    return pair_ids(jax.random.fold_in(key, 23), CAP_T, TB_DEV)


def shard_levels(stream_key, shape, pieces, least, largest):
    gain = 1.0
    for dim, parts in pieces:
        draws = jax.random.uniform(jax.random.fold_in(jax.random.fold_in(stream_key, 6), dim), (parts,), jnp.float32, least / len(pieces), largest / len(pieces))
        gain = gain * jnp.repeat(jnp.exp(draws), shape[dim] // parts).reshape((-1,) + (1,) * (len(shape) - 1 - dim))
    return gain


def centred(own_key, shape, scale, most, cuts=(), kind=jnp.bfloat16):
    gain = shard_levels(own_key, shape, cuts, -0.22, 0.18) if cuts else 1.0
    array = jax.random.normal(own_key, shape, jnp.float32) * scale * gain
    return jnp.minimum(jnp.maximum(array, -most), most).astype(kind)


def setup_inputs(seed: int = 0) -> dict:
    splits = jax.random.split(jax.random.key(seed), 5)
    return {
        "source_field": centred(splits[0], (NSB, BLK, CH), 1.0, 6.0, ((0, 32),)),
        "weight_blocks": centred(splits[1], (NW, BLK, BLK), (BLK * WB_DEV // TB_DEV) ** -0.5, 0.1875, ((0, 32),)),
        "source_ids": draw_source_ids(jax.random.fold_in(splits[4], 71), 0),
        "target_ids": draw_target_ids(jax.random.fold_in(splits[4], 71), 0),
    }


def reference(source_field, weight_blocks, source_ids, target_ids):
    devices = N_GX * N_GY
    total = jnp.zeros((TB_DEV * devices, BLK, CH), jnp.float32)

    def accumulate(carry, index):
        start = (index * WB_DEV).astype(jnp.int32)
        weights = lax.dynamic_slice_in_dim(weight_blocks, start, WB_DEV, 0)
        src_rows = lax.dynamic_slice_in_dim(source_ids, start, WB_DEV, 0)
        tgt_rows = lax.dynamic_slice_in_dim(target_ids, start, WB_DEV, 0)
        gathered = source_field[src_rows]
        partial_value = jnp.einsum("kts,ksc->ktc", weights.astype(jnp.float32), gathered.astype(jnp.float32))
        return carry.at[tgt_rows].add(partial_value), None

    total, _ = lax.scan(accumulate, total, jnp.arange(devices, dtype=jnp.int32))
    return total.astype(jnp.bfloat16)
```

```python
import jax
import jax.numpy as jnp
from jax import lax
from jax.experimental import pallas as pl
from jax.experimental.pallas import tpu as pltpu
from jax.sharding import PartitionSpec as P

HALF = 2
TB_DEV = 64
CAP_S = 64
CAP_T = 16
AXES = ("gx", "gy")
NEAR = (-1, 1)
FAR = (-2, 2)
GROUP = 8
RING = 32
AHEAD = 24


def passed_along(value, steps):
    count = lax.axis_size(AXES)
    initial, last = (max(0, -steps), min(count, count - steps))
    return lax.ppermute(value, AXES, [(source, source + steps) for source in range(initial, last)])


def rows_of(ids, device, devices, held):
    clamped = jnp.clip(device, 0, devices - 1)
    return lax.dynamic_slice_in_dim(ids, clamped * held, held, 0)


def asked_of_me(ids, senders, myself, devices, held, per_device):
    rows = jnp.stack([rows_of(ids, s, devices, held) for s in senders])
    local = rows - myself * per_device
    blocks = jnp.arange(per_device, dtype=jnp.int32)
    wanted = jnp.any(local[:, :, None] == blocks[None, None, :], axis=1)
    before = blocks[None, :] < blocks[:, None]
    rank = jnp.sum((wanted[:, None, :] & before[None]).astype(jnp.int32), axis=2)
    return wanted, rank


def ranked(key, row, per_device):
    span = 2 * HALF + 1
    cells = jnp.arange(span * per_device, dtype=jnp.int32)
    named = jnp.any(key[:, None] == cells[None, :], axis=0)
    below = named[None, :] & (cells[None, :] < key[:, None]) & (cells[None, :] >= row[:, None] * per_device)
    return jnp.sum(below.astype(jnp.int32), axis=1)


def pick_kernel(chosen, source, *outs):
    count = outs[0].shape[0]
    for n, out in enumerate(outs):
        def step(i, _, n=n, out=out):
            out[i] = source[chosen[n * count + i]]
            return 0
        lax.fori_loop(0, count, step, 0, unroll=4)


def pick(chosen, source, pieces):
    shape = (CAP_S,) + source.shape[1:]
    return pl.pallas_call(
        pick_kernel,
        out_shape=[jax.ShapeDtypeStruct(shape, source.dtype)] * pieces,
        grid_spec=pltpu.PrefetchScalarGridSpec(
            num_scalar_prefetch=1,
            grid=(),
            in_specs=[pl.BlockSpec(memory_space=pltpu.VMEM)],
            out_specs=[pl.BlockSpec(memory_space=pltpu.VMEM)] * pieces,
        ),
        compiler_params=pltpu.CompilerParams(vmem_limit_bytes=24 * 2**20),
        name="pick",
    )(chosen, source)


def phase(bounds, wlist, rows, slots, weights, pieces, start, acc_base, splits, name):
    total = weights.shape[0]
    tile = weights.shape[1:]
    acc_tile = (weights.shape[1], pieces[0].shape[2])
    table_rows = sum(p.shape[0] for p in pieces)
    acc_rows = sum(splits)
    n_pieces = len(pieces)
    n_start = 0 if start is None else 1

    def kernel(b, wl, ti, sl, w, *refs):
        piece_refs = refs[:n_pieces]
        start_refs = refs[n_pieces : n_pieces + n_start]
        outs = refs[n_pieces + n_start : n_pieces + n_start + len(splits)]
        table, acc, ring, sem_ring, sem_tab, sem_io = refs[n_pieces + n_start + len(splits) :]
        lo = b[0]
        hi = b[1]
        groups = (hi - lo + GROUP - 1) // GROUP

        loads = []
        offset = 0
        for n, p in enumerate(piece_refs):
            loads.append(
                pltpu.make_async_copy(p, table.at[pl.ds(offset, p.shape[0])], sem_tab.at[n])
            )
            offset += p.shape[0]
        if n_start:
            loads.append(
                pltpu.make_async_copy(start_refs[0], acc.at[pl.ds(0, acc_rows)], sem_tab.at[n_pieces])
            )
        for c in loads:
            c.start()

        def issue(g, _):
            slot = g % RING
            for j in range(GROUP):
                i = jnp.minimum(lo + g * GROUP + j, total - 1)
                pltpu.make_async_copy(
                    w.at[wl[i]], ring.at[slot * GROUP + j], sem_ring.at[slot]
                ).start()
            return 0

        lax.fori_loop(0, jnp.minimum(groups, AHEAD), issue, 0)
        if not n_start:
            def clear(i, _):
                acc[i] = jnp.zeros(acc_tile, jnp.float32)
                return 0
            lax.fori_loop(0, acc_rows + 1, clear, 0)
        for c in loads:
            c.wait()

        def step(g, _):
            @pl.when(g + AHEAD < groups)
            def _():
                issue(g + AHEAD, 0)
            slot = g % RING
            held = ring.at[pl.ds(slot * GROUP, GROUP)]
            pltpu.make_async_copy(w.at[pl.ds(0, GROUP)], held, sem_ring.at[slot]).wait()
            for j in range(GROUP):
                i = lo + g * GROUP + j
                inside = i < hi
                i = jnp.minimum(i, total - 1)
                where = jnp.where(inside, sl[i] - acc_base, acc_rows)
                row = jnp.where(inside, ti[i], 0)
                part = jnp.dot(ring[slot * GROUP + j], table[row], preferred_element_type=jnp.float32)
                acc[where] += part
            return 0

        lax.fori_loop(0, groups, step, 0)
        stores = []
        offset = 0
        for n, o in enumerate(outs):
            stores.append(pltpu.make_async_copy(acc.at[pl.ds(offset, splits[n])], o, sem_io.at[n]))
            offset += splits[n]
        for c in stores:
            c.start()
        for c in stores:
            c.wait()

    anywhere = pl.BlockSpec(memory_space=pl.ANY)
    return pl.pallas_call(
        kernel,
        out_shape=[jax.ShapeDtypeStruct((n,) + acc_tile, jnp.float32) for n in splits],
        grid_spec=pltpu.PrefetchScalarGridSpec(
            num_scalar_prefetch=4,
            grid=(),
            in_specs=[anywhere] * (1 + n_pieces + n_start),
            out_specs=[anywhere] * len(splits),
            scratch_shapes=[
                pltpu.VMEM((table_rows,) + pieces[0].shape[1:], pieces[0].dtype),
                pltpu.VMEM((acc_rows + 1,) + acc_tile, jnp.float32),
                pltpu.VMEM((RING * GROUP,) + tile, weights.dtype),
                pltpu.SemaphoreType.DMA((RING,)),
                pltpu.SemaphoreType.DMA((n_pieces + 1,)),
                pltpu.SemaphoreType.DMA((len(splits),)),
            ],
        ),
        compiler_params=pltpu.CompilerParams(vmem_limit_bytes=40 * 2**20),
        name=name,
    )(bounds, wlist, rows, slots, weights, *pieces, *([] if start is None else [start]))


def combine(places, boxes, out_rows):
    tile = boxes[0].shape[1:]
    held = sum(b.shape[0] for b in boxes)
    count = len(boxes)

    def kernel(pl_ref, *refs):
        ins = refs[:count]
        out, buf, sems = refs[count:]
        loads = []
        offset = 0
        for n, r in enumerate(ins):
            loads.append(pltpu.make_async_copy(r, buf.at[pl.ds(offset, r.shape[0])], sems.at[n]))
            offset += r.shape[0]
        for c in loads:
            c.start()
        buf[held] = jnp.zeros(tile, jnp.float32)
        for c in loads:
            c.wait()

        def step(t, _):
            total = buf[pl_ref[t]]
            for n in range(1, count):
                total = total + buf[pl_ref[n * out_rows + t]]
            out[t] = total.astype(jnp.bfloat16)
            return 0

        lax.fori_loop(0, out_rows, step, 0, unroll=2)

    return pl.pallas_call(
        kernel,
        out_shape=jax.ShapeDtypeStruct((out_rows,) + tile, jnp.bfloat16),
        grid_spec=pltpu.PrefetchScalarGridSpec(
            num_scalar_prefetch=1,
            grid=(),
            in_specs=[pl.BlockSpec(memory_space=pl.ANY)] * count,
            out_specs=pl.BlockSpec(memory_space=pltpu.VMEM),
            scratch_shapes=[
                pltpu.VMEM((held + 1,) + tile, jnp.float32),
                pltpu.SemaphoreType.DMA((count,)),
            ],
        ),
        compiler_params=pltpu.CompilerParams(vmem_limit_bytes=24 * 2**20),
        name="combine",
    )(places, *boxes)


def body(source_field, weight_blocks, source_ids, target_ids):
    devices = lax.axis_size(AXES)
    myself = lax.axis_index(AXES)
    held = weight_blocks.shape[0]
    src_count = source_field.shape[0]

    def outgoing(rels):
        wanted, rank = asked_of_me(
            source_ids, [myself - r for r in rels], myself, devices, held, src_count
        )
        slots = jnp.arange(CAP_S, dtype=jnp.int32)
        blocks = jnp.arange(src_count, dtype=jnp.int32)
        match = wanted[:, None, :] & (rank[:, None, :] == slots[None, :, None])
        chosen = jnp.sum(jnp.where(match, blocks[None, None, :], 0), axis=2)
        return pick(chosen.reshape(-1), source_field, len(rels))

    near = [passed_along(p, -r) for r, p in zip(NEAR, outgoing(NEAR))]
    far = [passed_along(p, -r) for r, p in zip(FAR, outgoing(FAR))]

    own_src = rows_of(source_ids, myself, devices, held)
    src_rel = own_src // src_count - myself
    src_local = own_src % src_count
    src_row = src_rel + HALF
    src_rank = ranked(src_row * src_count + src_local, src_row, src_count)
    row = jnp.where(
        src_rel == 0,
        src_local,
        jnp.where(
            jnp.abs(src_rel) == 1,
            src_count + jnp.where(src_rel > 0, CAP_S, 0) + src_rank,
            jnp.where(src_rel > 0, CAP_S, 0) + src_rank,
        ),
    )
    own_tgt = rows_of(target_ids, myself, devices, held)
    tgt_rel = own_tgt // TB_DEV - myself
    tgt_row = tgt_rel + HALF
    tgt_rank = ranked(tgt_row * TB_DEV + own_tgt % TB_DEV, tgt_row, TB_DEV)
    bucket = jnp.where(
        tgt_rel == 0,
        4,
        jnp.where(jnp.abs(tgt_rel) == 1, 2, 0) + jnp.where(tgt_rel > 0, 1, 0),
    )
    slot = bucket * CAP_T + tgt_rank
    n_slots = (2 * HALF + 1) * CAP_T
    part = jnp.where(jnp.abs(src_rel) < 2, 0, jnp.where(jnp.abs(tgt_rel) == 2, 1, 2))
    order_key = (part * n_slots + slot) * held + jnp.arange(held, dtype=jnp.int32)
    position = jnp.sum((order_key[None, :] < order_key[:, None]).astype(jnp.int32), axis=1)
    hit = position[None, :] == jnp.arange(held, dtype=jnp.int32)[:, None]
    ks = jnp.arange(held, dtype=jnp.int32)
    wlist = jnp.sum(jnp.where(hit, ks[None, :], 0), axis=1)
    rows = jnp.sum(jnp.where(hit, row[None, :], 0), axis=1)
    slots = jnp.sum(jnp.where(hit, slot[None, :], 0), axis=1)
    ends = jnp.sum((part[None, :] <= jnp.arange(3, dtype=jnp.int32)[:, None]).astype(jnp.int32), axis=1)
    zero = jnp.zeros((1,), jnp.int32)

    first = phase(
        jnp.concatenate([zero, ends[:1]]), wlist, rows, slots, weight_blocks,
        [source_field] + near, None, 0, (2 * CAP_T, 3 * CAP_T), "near_products",
    )
    to_far = phase(
        ends[0:2], wlist, rows, slots, weight_blocks, far, first[0], 0,
        (CAP_T, CAP_T), "far_products",
    )
    last_bounds, to_far = lax.optimization_barrier((ends[1:3], to_far))
    far_boxes = [passed_along(b, r) for r, b in zip(FAR, to_far)]
    rest = phase(
        last_bounds, wlist, rows, slots, weight_blocks, far, first[1], 2 * CAP_T,
        (CAP_T, CAP_T, CAP_T), "rest_products",
    )
    near_boxes = [passed_along(b, r) for r, b in zip(NEAR, rest[:2])]

    senders = [myself - r for r in FAR + NEAR + (0,)]
    wanted, rank = asked_of_me(target_ids, senders, myself, devices, held, TB_DEV)
    sender = jnp.stack(senders)
    valid = wanted & ((sender >= 0) & (sender < devices))[:, None]
    box = jnp.arange(len(senders), dtype=jnp.int32)[:, None] * CAP_T
    places = jnp.where(valid, box + rank, n_slots).reshape(-1)
    return combine(places, far_boxes + near_boxes + [rest[2]], TB_DEV)


def solution(mesh):
    return jax.shard_map(
        body,
        mesh=mesh,
        in_specs=(P(AXES, None, None), P(AXES, None, None), P(), P()),
        out_specs=P(AXES, None, None),
        check_vma=False,
    )
```

```python
import jax
import jax.numpy as jnp
from jax import lax
from jax.experimental import pallas as pl
from jax.experimental.pallas import tpu as pltpu
from jax.sharding import PartitionSpec as P

HALF = 2
TB_DEV = 64
CAP_S = 64
CAP_T = 16
AXES = ("gx", "gy")
NEAR = (-1, 1)
FAR = (-2, 2)
GROUP = 8
RING = 32
AHEAD = 24


def passed_along(value, steps):
    count = lax.axis_size(AXES)
    initial, last = (max(0, -steps), min(count, count - steps))
    return lax.ppermute(value, AXES, [(source, source + steps) for source in range(initial, last)])


def rows_of(ids, device, devices, held):
    clamped = jnp.clip(device, 0, devices - 1)
    return lax.dynamic_slice_in_dim(ids, clamped * held, held, 0)


def asked_of_me(ids, senders, myself, devices, held, per_device):
    rows = jnp.stack([rows_of(ids, s, devices, held) for s in senders])
    local = rows - myself * per_device
    blocks = jnp.arange(per_device, dtype=jnp.int32)
    wanted = jnp.any(local[:, :, None] == blocks[None, None, :], axis=1)
    before = blocks[None, :] < blocks[:, None]
    rank = jnp.sum((wanted[:, None, :] & before[None]).astype(jnp.int32), axis=2)
    return wanted, rank


def ranked(key, row, per_device):
    span = 2 * HALF + 1
    cells = jnp.arange(span * per_device, dtype=jnp.int32)
    named = jnp.any(key[:, None] == cells[None, :], axis=0)
    below = named[None, :] & (cells[None, :] < key[:, None]) & (cells[None, :] >= row[:, None] * per_device)
    return jnp.sum(below.astype(jnp.int32), axis=1)


def pick_kernel(chosen, source, *outs):
    count = outs[0].shape[0]
    for n, out in enumerate(outs):
        def step(i, _, n=n, out=out):
            out[i] = source[chosen[n * count + i]]
            return 0
        lax.fori_loop(0, count, step, 0, unroll=4)


def pick(chosen, source, pieces):
    shape = (CAP_S,) + source.shape[1:]
    return pl.pallas_call(
        pick_kernel,
        out_shape=[jax.ShapeDtypeStruct(shape, source.dtype)] * pieces,
        grid_spec=pltpu.PrefetchScalarGridSpec(
            num_scalar_prefetch=1,
            grid=(),
            in_specs=[pl.BlockSpec(memory_space=pltpu.VMEM)],
            out_specs=[pl.BlockSpec(memory_space=pltpu.VMEM)] * pieces,
        ),
        compiler_params=pltpu.CompilerParams(vmem_limit_bytes=24 * 2**20),
        name="pick",
    )(chosen, source)


def phase(bounds, wlist, rows, slots, weights, pieces, start, acc_base, splits, name):
    total = weights.shape[0]
    tile = weights.shape[1:]
    acc_tile = (weights.shape[1], pieces[0].shape[2])
    table_rows = sum(p.shape[0] for p in pieces)
    acc_rows = sum(splits)
    n_pieces = len(pieces)
    n_start = 0 if start is None else 1

    def kernel(b, wl, ti, sl, w, *refs):
        piece_refs = refs[:n_pieces]
        start_refs = refs[n_pieces : n_pieces + n_start]
        outs = refs[n_pieces + n_start : n_pieces + n_start + len(splits)]
        table, acc, ring, sem_ring, sem_tab, sem_io = refs[n_pieces + n_start + len(splits) :]
        lo = b[0]
        hi = b[1]
        groups = (hi - lo + GROUP - 1) // GROUP

        loads = []
        offset = 0
        for n, p in enumerate(piece_refs):
            loads.append(
                pltpu.make_async_copy(p, table.at[pl.ds(offset, p.shape[0])], sem_tab.at[n])
            )
            offset += p.shape[0]
        if n_start:
            loads.append(
                pltpu.make_async_copy(start_refs[0], acc.at[pl.ds(0, acc_rows)], sem_tab.at[n_pieces])
            )
        for c in loads:
            c.start()

        def issue(g, _):
            slot = g % RING
            for j in range(GROUP):
                i = jnp.minimum(lo + g * GROUP + j, total - 1)
                pltpu.make_async_copy(
                    w.at[wl[i]], ring.at[slot * GROUP + j], sem_ring.at[slot]
                ).start()
            return 0

        lax.fori_loop(0, jnp.minimum(groups, AHEAD), issue, 0)
        if not n_start:
            def clear(i, _):
                acc[i] = jnp.zeros(acc_tile, jnp.float32)
                return 0
            lax.fori_loop(0, acc_rows + 1, clear, 0)
        for c in loads:
            c.wait()

        def step(g, _):
            @pl.when(g + AHEAD < groups)
            def _():
                issue(g + AHEAD, 0)
            slot = g % RING
            held = ring.at[pl.ds(slot * GROUP, GROUP)]
            pltpu.make_async_copy(w.at[pl.ds(0, GROUP)], held, sem_ring.at[slot]).wait()
            for j in range(GROUP):
                i = lo + g * GROUP + j
                inside = i < hi
                i = jnp.minimum(i, total - 1)
                where = jnp.where(inside, sl[i] - acc_base, acc_rows)
                row = jnp.where(inside, ti[i], 0)
                part = jnp.dot(ring[slot * GROUP + j], table[row], preferred_element_type=jnp.float32)
                acc[where] += part
            return 0

        lax.fori_loop(0, groups, step, 0)
        stores = []
        offset = 0
        for n, o in enumerate(outs):
            stores.append(pltpu.make_async_copy(acc.at[pl.ds(offset, splits[n])], o, sem_io.at[n]))
            offset += splits[n]
        for c in stores:
            c.start()
        for c in stores:
            c.wait()

    anywhere = pl.BlockSpec(memory_space=pl.ANY)
    return pl.pallas_call(
        kernel,
        out_shape=[jax.ShapeDtypeStruct((n,) + acc_tile, jnp.float32) for n in splits],
        grid_spec=pltpu.PrefetchScalarGridSpec(
            num_scalar_prefetch=4,
            grid=(),
            in_specs=[anywhere] * (1 + n_pieces + n_start),
            out_specs=[anywhere] * len(splits),
            scratch_shapes=[
                pltpu.VMEM((table_rows,) + pieces[0].shape[1:], pieces[0].dtype),
                pltpu.VMEM((acc_rows + 1,) + acc_tile, jnp.float32),
                pltpu.VMEM((RING * GROUP,) + tile, weights.dtype),
                pltpu.SemaphoreType.DMA((RING,)),
                pltpu.SemaphoreType.DMA((n_pieces + 1,)),
                pltpu.SemaphoreType.DMA((len(splits),)),
            ],
        ),
        compiler_params=pltpu.CompilerParams(vmem_limit_bytes=40 * 2**20),
        name=name,
    )(bounds, wlist, rows, slots, weights, *pieces, *([] if start is None else [start]))


def combine(places, boxes, out_rows):
    tile = boxes[0].shape[1:]
    held = sum(b.shape[0] for b in boxes)
    count = len(boxes)

    def kernel(pl_ref, *refs):
        ins = refs[:count]
        out, buf, sems = refs[count:]
        loads = []
        offset = 0
        for n, r in enumerate(ins):
            loads.append(pltpu.make_async_copy(r, buf.at[pl.ds(offset, r.shape[0])], sems.at[n]))
            offset += r.shape[0]
        for c in loads:
            c.start()
        buf[held] = jnp.zeros(tile, jnp.float32)
        for c in loads:
            c.wait()

        def step(t, _):
            total = buf[pl_ref[t]]
            for n in range(1, count):
                total = total + buf[pl_ref[n * out_rows + t]]
            out[t] = total.astype(jnp.bfloat16)
            return 0

        lax.fori_loop(0, out_rows, step, 0, unroll=2)

    return pl.pallas_call(
        kernel,
        out_shape=jax.ShapeDtypeStruct((out_rows,) + tile, jnp.bfloat16),
        grid_spec=pltpu.PrefetchScalarGridSpec(
            num_scalar_prefetch=1,
            grid=(),
            in_specs=[pl.BlockSpec(memory_space=pl.ANY)] * count,
            out_specs=pl.BlockSpec(memory_space=pltpu.VMEM),
            scratch_shapes=[
                pltpu.VMEM((held + 1,) + tile, jnp.float32),
                pltpu.SemaphoreType.DMA((count,)),
            ],
        ),
        compiler_params=pltpu.CompilerParams(vmem_limit_bytes=24 * 2**20),
        name="combine",
    )(places, *boxes)


def body(source_field, weight_blocks, source_ids, target_ids):
    devices = lax.axis_size(AXES)
    myself = lax.axis_index(AXES)
    held = weight_blocks.shape[0]
    src_count = source_field.shape[0]

    def picked(field, dests, owner):
        wanted, rank = asked_of_me(source_ids, dests, owner, devices, held, src_count)
        slots = jnp.arange(CAP_S, dtype=jnp.int32)
        blocks = jnp.arange(src_count, dtype=jnp.int32)
        match = wanted[:, None, :] & (rank[:, None, :] == slots[None, :, None])
        chosen = jnp.sum(jnp.where(match, blocks[None, None, :], 0), axis=2)
        return pick(chosen.reshape(-1), field, len(dests))

    relayed = lax.axis_size("gy") == 2 * HALF
    if relayed:
        n_gx = lax.axis_size("gx")
        line = lax.axis_index("gy")
        far_sign = jnp.where(line < HALF, 1, -1)
        near_sign = jnp.where(line % 2 == 0, 1, -1)
        n_gy = 2 * HALF
        half_pairs, near_pairs, same_pairs, turn_pairs = [], [], [], []
        for g in range(n_gx):
            for z in range(n_gy):
                d = g * n_gy + z
                way = 1 if z < HALF else -1
                half_pairs.append((d, d + 2 * way))
                near_pairs.append((d, d + 1 - 2 * (z % 2)))
                if 0 <= g + way < n_gx:
                    same_pairs.append((d, d + n_gy * way))
                to = d + (1, 3, -3, -1)[z]
                if 0 <= to < n_gx * n_gy:
                    turn_pairs.append((d, to))
        turn_step = jnp.where(line == 0, 1, jnp.where(line == 1, 3, jnp.where(line == 2, -3, -1)))
        crossed = lax.ppermute(source_field, AXES, half_pairs)
        (beside,) = picked(source_field, [myself + near_sign], myself)
        near = [lax.ppermute(beside, AXES, near_pairs)]
        turn, same = picked(
            crossed, [myself + turn_step, myself + n_gy * far_sign], myself + 2 * far_sign
        )
        far = [
            crossed,
            lax.ppermute(turn, AXES, turn_pairs),
            lax.ppermute(same, AXES, same_pairs),
        ]
    else:
        near, far = (
            [
                passed_along(p, -r)
                for r, p in zip(rels, picked(source_field, [myself - r for r in rels], myself))
            ]
            for rels in (NEAR, FAR)
        )

    own_src = rows_of(source_ids, myself, devices, held)
    src_rel = own_src // src_count - myself
    src_local = own_src % src_count
    src_row = src_rel + HALF
    src_rank = ranked(src_row * src_count + src_local, src_row, src_count)
    if relayed:
        beside_me = src_rel == near_sign
        late = (src_rel != 0) & ~beside_me
        row = jnp.where(
            (src_rel == 0) | (src_rel == 2 * far_sign),
            src_local,
            src_count + src_rank + jnp.where(src_rel == -2 * far_sign, CAP_S, 0),
        )
    else:
        late = jnp.abs(src_rel) == 2
        row = jnp.where(
            src_rel == 0,
            src_local,
            jnp.where(late, 0, src_count) + jnp.where(src_rel > 0, CAP_S, 0) + src_rank,
        )
    own_tgt = rows_of(target_ids, myself, devices, held)
    tgt_rel = own_tgt // TB_DEV - myself
    tgt_row = tgt_rel + HALF
    tgt_rank = ranked(tgt_row * TB_DEV + own_tgt % TB_DEV, tgt_row, TB_DEV)
    bucket = jnp.where(
        tgt_rel == 0,
        4,
        jnp.where(jnp.abs(tgt_rel) == 1, 2, 0) + jnp.where(tgt_rel > 0, 1, 0),
    )
    slot = bucket * CAP_T + tgt_rank
    n_slots = (2 * HALF + 1) * CAP_T
    part = jnp.where(~late, 0, jnp.where(jnp.abs(tgt_rel) == 2, 1, 2))
    order_key = (part * n_slots + slot) * held + jnp.arange(held, dtype=jnp.int32)
    position = jnp.sum((order_key[None, :] < order_key[:, None]).astype(jnp.int32), axis=1)
    hit = position[None, :] == jnp.arange(held, dtype=jnp.int32)[:, None]
    ks = jnp.arange(held, dtype=jnp.int32)
    wlist = jnp.sum(jnp.where(hit, ks[None, :], 0), axis=1)
    rows = jnp.sum(jnp.where(hit, row[None, :], 0), axis=1)
    slots = jnp.sum(jnp.where(hit, slot[None, :], 0), axis=1)
    ends = jnp.sum((part[None, :] <= jnp.arange(3, dtype=jnp.int32)[:, None]).astype(jnp.int32), axis=1)
    zero = jnp.zeros((1,), jnp.int32)

    first = phase(
        jnp.concatenate([zero, ends[:1]]), wlist, rows, slots, weight_blocks,
        [source_field] + near, None, 0, (2 * CAP_T, 3 * CAP_T), "near_products",
    )
    to_far = phase(
        ends[0:2], wlist, rows, slots, weight_blocks, far, first[0], 0,
        (CAP_T, CAP_T), "far_products",
    )
    last_bounds, to_far = lax.optimization_barrier((ends[1:3], to_far))
    far_boxes = [passed_along(b, r) for r, b in zip(FAR, to_far)]
    rest = phase(
        last_bounds, wlist, rows, slots, weight_blocks, far, first[1], 2 * CAP_T,
        (CAP_T, CAP_T, CAP_T), "rest_products",
    )
    near_boxes = [passed_along(b, r) for r, b in zip(NEAR, rest[:2])]

    senders = [myself - r for r in FAR + NEAR + (0,)]
    wanted, rank = asked_of_me(target_ids, senders, myself, devices, held, TB_DEV)
    sender = jnp.stack(senders)
    valid = wanted & ((sender >= 0) & (sender < devices))[:, None]
    box = jnp.arange(len(senders), dtype=jnp.int32)[:, None] * CAP_T
    places = jnp.where(valid, box + rank, n_slots).reshape(-1)
    return combine(places, far_boxes + near_boxes + [rest[2]], TB_DEV)


def solution(mesh):
    return jax.shard_map(
        body,
        mesh=mesh,
        in_specs=(P(AXES, None, None), P(AXES, None, None), P(), P()),
        out_specs=P(AXES, None, None),
        check_vma=False,
    )
```
